32 devices in a mesh: segment: 4 (over z), tok: 4 (over y, x), mp: 2 (over core).
Axes of the slice: x: 2, y: 2, z: 4, core: 2. Of those that a mesh axis runs over, the one named last changes fastest.
Arguments:
- out_cotangent: bfloat16 [4, 512, 4096], P('segment', 'tok', 'mp'), may hold values from -6 to 6
- block_output: bfloat16 [4, 512, 4096], P('segment', 'tok', 'mp'), may hold values from -6 to 6
- router_logits: float32 [4, 512], P('segment', 'tok'), may hold values from -8 to 8
- keep_flags: int32 [4, 512], P('segment', 'tok'), may hold values from 0 to 1, as said below
- router_weight: float32 [4, 4096], P('segment', 'mp'), may hold values from -0.09375 to 0.09375
- activated: bfloat16 [4, 64, 14336], P('segment', None, 'tok'), may hold values from -4 to 4
Outputs:
- cotangent_received: bfloat16 [4, 512, 4096], P('segment', 'tok', 'mp')
- grad_out: bfloat16 [4, 4096, 14336], P('segment', 'mp', 'tok')
The draws below stay inside these ranges and needn't reach their ends.
Inputs may be any that keep to these rules, and one draw needn't show every extreme that they name: `keep_flags`: in every segment each aligned block of 128 tokens (one device of a group) holds at most 48 active tokens, some block holds exactly 48, and the segment holds exactly 64 active tokens.
All inputs are finite; a program needn't handle non-finite values.
Results may differ from the reference program's by a relative error of at most 0.0049.
Values may be sent and summed in bfloat16 or wider, within the bound.
No kernel may reach another device: no remote copies, remote signals or barrier semaphores. Data moves between devices by JAX's collectives and lax.ppermute only.
A program may use at most 64 MiB of HBM per device.

```python
import jax
import jax.numpy as jnp
from jax import lax

D = 4096
HID = 14336
TOK_DEV = 128
TOKENS = 512
GROUP_ACTIVE = 64
RELAY_SECTIONS = 4


def draw_keep_flags(key, part):
    token_groups = TOKENS // TOK_DEV
    average = TOK_DEV // 8
    largest_row_count = 3 * average
    key_weight = jax.random.fold_in(key, 11)
    key_heavy = jax.random.fold_in(key, 12)
    key_extra = jax.random.fold_in(key, 13)
    key_place = jax.random.fold_in(key, 14)
    weights = jax.random.randint(key_weight, (RELAY_SECTIONS, token_groups), 2, 5)
    heaviest = jax.random.randint(key_heavy, (RELAY_SECTIONS, 1), 0, token_groups)
    device_index = jnp.arange(token_groups, dtype=jnp.int32)[None, :]
    heavy_flag = device_index == heaviest
    weights = jnp.where(heavy_flag, 0, weights)
    remainder = token_groups * average - largest_row_count
    weight_sum = jnp.sum(weights, axis=1, keepdims=True)
    row_shares = remainder * weights // weight_sum
    spare_rows = remainder - jnp.sum(row_shares, axis=1, keepdims=True)
    within_remaining = device_index - (device_index > heaviest).astype(jnp.int32)
    cyclic_shift = jax.random.randint(key_extra, (RELAY_SECTIONS, 1), 0, token_groups - 1)
    extra_row = (jnp.mod(within_remaining + cyclic_shift, token_groups - 1) < spare_rows).astype(jnp.int32)
    row_count_list = jnp.where(heavy_flag, largest_row_count, row_shares + extra_row)
    row_keys = jax.random.split(key_place, RELAY_SECTIONS * token_groups)
    token_rank = jax.vmap(lambda one_key: jax.random.permutation(one_key, TOK_DEV))(row_keys)
    token_rank = token_rank.reshape(RELAY_SECTIONS, token_groups, TOK_DEV)
    keep_flags = (token_rank < row_count_list[:, :, None]).astype(jnp.int32)
    return keep_flags.reshape(RELAY_SECTIONS, TOKENS)


def levels(stream_key, dims, pieces, low, largest):
    level, own = 1.0, jax.random.fold_in(stream_key, 6)
    for dim, shards_of in pieces:
        heights = jnp.exp(jax.random.uniform(jax.random.fold_in(own, dim), (shards_of,), jnp.float32, low / len(pieces), largest / len(pieces)))
        level = level * jnp.repeat(heights, dims[dim] // shards_of).reshape([-1 if axis == dim else 1 for axis in range(len(dims))])
    return level


def scatter_about(stream_key, dims, width, most, cuts=(), kind=jnp.bfloat16):
    result = width * jax.random.normal(stream_key, dims, jnp.float32)
    if cuts:
        result = result * levels(stream_key, dims, cuts, -0.22, 0.18)
    return jnp.clip(result, -most, most).astype(kind)


def setup_inputs(seed: int = 0) -> dict:
    keys = jax.random.split(jax.random.key(seed), 7)
    out_cotangent = scatter_about(keys[0], (RELAY_SECTIONS, TOKENS, D), 1.0, 6.0, ((0, 4), (1, 4), (2, 2)))
    block_output = scatter_about(keys[1], (RELAY_SECTIONS, TOKENS, D), 1.0, 6.0, ((0, 4), (1, 4), (2, 2)))
    router_logits = scatter_about(keys[2], (RELAY_SECTIONS, TOKENS), 2.0, 8.0, ((0, 4), (1, 4)), jnp.float32)
    keep_flags = draw_keep_flags(jax.random.fold_in(keys[6], 71), 0)
    router_weight = scatter_about(keys[4], (RELAY_SECTIONS, D), D ** -0.5, 0.09375, ((0, 4), (1, 2)), jnp.float32)
    activated = scatter_about(keys[5], (RELAY_SECTIONS, GROUP_ACTIVE, HID), 0.25, 4.0, ((0, 4), (2, 4)))
    return {"out_cotangent": out_cotangent, "block_output": block_output, "router_logits": router_logits, "keep_flags": keep_flags, "router_weight": router_weight, "activated": activated}


def segment_part(cotangent, output, keep_row, logits, router_row, stored):
    dy_float = cotangent.astype(jnp.float32)
    gate_value = jax.nn.sigmoid(logits)
    grad_gate = jnp.sum(dy_float * output.astype(jnp.float32), axis=1)
    grad_score = keep_row.astype(jnp.float32) * grad_gate * gate_value * (1.0 - gate_value)
    dx_tokens = (dy_float + grad_score[:, None] * router_row[None, :]).astype(jnp.bfloat16)
    order = jnp.argsort(1 - keep_row, stable=True)[:GROUP_ACTIVE].astype(jnp.int32)
    dz_rows = (jnp.take(gate_value, order)[:, None] * jnp.take(dy_float, order, axis=0)).astype(jnp.bfloat16)
    gradient = jnp.dot(dz_rows.T, stored, preferred_element_type=jnp.float32).astype(jnp.bfloat16)
    return dx_tokens, gradient


def reference(out_cotangent, block_output, router_logits, keep_flags, router_weight, activated):
    def apply_segment(members):
        return segment_part(members[0], members[1], members[2], members[3], members[4], members[5])

    dx_all, grad_out = lax.map(apply_segment, (out_cotangent, block_output, keep_flags, router_logits, router_weight, activated))
    received = jnp.concatenate([dx_all[1:], jnp.zeros_like(dx_all[:1])], axis=0)
    return received, grad_out
```

```python
import functools

import jax
import jax.numpy as jnp
from jax import lax
from jax.experimental import pallas as pl
from jax.experimental.pallas import tpu as pltpu
from jax.sharding import PartitionSpec as P


CAP = 48
LANES = 128
PIECES = 2
BLOCK = 128
LEFT = 4
MIB = 1024 * 1024

VMEM = pl.BlockSpec(memory_space=pltpu.VMEM)
ANY = pl.BlockSpec(memory_space=pl.ANY)
HBM = pl.BlockSpec(memory_space=pltpu.HBM)


def widths_of(features):
    first = features * 5 // 8 // BLOCK * BLOCK
    return [first, features - first]


def prepare_kernel(widths, cot_hbm, out_hbm, logit_hbm, keep_hbm, weight_hbm, stored_hbm, *refs):
    rows_refs = refs[: len(widths)]
    score_ref, weight_ref, stored_ref, cot_ref, out_ref, logit_ref, keep_ref, sems = refs[
        len(widths) :
    ]
    pairs = [
        (logit_hbm, logit_ref),
        (keep_hbm, keep_ref),
        (cot_hbm, cot_ref),
        (out_hbm, out_ref),
        (weight_hbm, weight_ref),
        (stored_hbm, stored_ref),
    ]
    copies = [
        pltpu.make_async_copy(source, target, sems.at[index])
        for index, (source, target) in enumerate(pairs)
    ]
    for copy in copies:
        copy.start()
    tokens = cot_ref.shape[0]
    upper = (
        lax.broadcasted_iota(jnp.int32, (tokens, tokens), 0)
        <= lax.broadcasted_iota(jnp.int32, (tokens, tokens), 1)
    ).astype(jnp.float32).astype(jnp.bfloat16)
    copies[0].wait()
    copies[1].wait()
    keep = keep_ref[...]
    gate = jax.nn.sigmoid(logit_ref[...])
    keep_half = jnp.broadcast_to(keep.astype(jnp.float32), (16, tokens)).astype(jnp.bfloat16)
    rank = jnp.dot(keep_half, upper, preferred_element_type=jnp.float32)[:1]
    slot = lax.broadcasted_iota(jnp.int32, (CAP, tokens), 0) + 1
    chosen = (rank.astype(jnp.int32) == slot) & (keep > 0)
    gate_column = jnp.sum(jnp.where(chosen, gate, 0.0), axis=1, keepdims=True)
    chooser = jnp.where(chosen, 1.0, 0.0).astype(jnp.bfloat16)
    count = jnp.sum(keep.astype(jnp.float32), axis=1, keepdims=True)
    copies[2].wait()
    start = 0
    for index, (ref, width) in enumerate(zip(rows_refs, widths)):
        picked = jnp.dot(
            chooser, cot_ref[:, start : start + width], preferred_element_type=jnp.float32
        )
        ref[:, :width] = (picked * gate_column).astype(jnp.bfloat16)
        if index == 0:
            ref[:, width:] = jnp.broadcast_to(count, (CAP, LANES)).astype(jnp.bfloat16)
        start += width
    copies[3].wait()
    folded = jnp.zeros((tokens, LANES), jnp.float32)
    for start in range(0, cot_ref.shape[1], LANES):
        folded = folded + (
            cot_ref[:, start : start + LANES].astype(jnp.float32)
            * out_ref[:, start : start + LANES].astype(jnp.float32)
        )
    part = jnp.sum(folded.T, axis=0, keepdims=True)
    score_ref[...] = keep.astype(jnp.float32) * part * gate * (1.0 - gate)
    copies[4].wait()
    copies[5].wait()


def prepare(cotangent, output, logits, keep_row, weight, stored):
    widths = widths_of(cotangent.shape[1])
    return pl.pallas_call(
        functools.partial(prepare_kernel, widths),
        in_specs=[HBM] * 6,
        out_specs=[VMEM] * (len(widths) + 3),
        out_shape=[
            pltpu.VMEM((CAP, width + (LANES if index == 0 else 0)), jnp.bfloat16)
            for index, width in enumerate(widths)
        ]
        + [
            pltpu.VMEM(logits.shape, jnp.float32),
            pltpu.VMEM(weight.shape, jnp.float32),
            pltpu.VMEM(stored.shape, jnp.bfloat16),
        ],
        scratch_shapes=[
            pltpu.VMEM(cotangent.shape, jnp.bfloat16),
            pltpu.VMEM(output.shape, jnp.bfloat16),
            pltpu.VMEM(logits.shape, jnp.float32),
            pltpu.VMEM(keep_row.shape, jnp.int32),
            pltpu.SemaphoreType.DMA((6,)),
        ],
        compiler_params=pltpu.CompilerParams(vmem_limit_bytes=8 * MIB),
        name="prepare",
    )(*[
        pltpu.with_memory_space_constraint(x, pltpu.HBM)
        for x in (cotangent, output, logits, keep_row, weight, stored)
    ])


def place_of(row_refs, width, total):
    group = len(row_refs)
    me = lax.axis_index("tok")
    counts = [ref[:1, width : width + LANES].astype(jnp.float32)[:, :CAP] for ref in row_refs]
    owners = [partner(me, r, group) for r in range(group)]
    lane = lax.broadcasted_iota(jnp.int32, (total, CAP), 1)
    target = lax.broadcasted_iota(jnp.int32, (total, CAP), 0)
    places = []
    for r in range(group):
        offset = jnp.zeros_like(counts[0])
        for other in range(group):
            if other != r:
                ahead = (owners[other] < owners[r]).astype(jnp.float32)
                offset = offset + counts[other] * ahead
        place = (offset.astype(jnp.int32) + lane == target) & (lane < counts[r].astype(jnp.int32))
        places.append(jnp.where(place, 1.0, 0.0).astype(jnp.bfloat16))
    return places


def pack_rows(row_refs, places, lhs_ref):
    width = lhs_ref.shape[0]
    packed = None
    for place, ref in zip(places, row_refs):
        one = jnp.dot(place, ref[:, :width], preferred_element_type=jnp.float32)
        packed = one if packed is None else packed + one
    lhs_ref[...] = packed.T.astype(jnp.bfloat16)


def product(lhs_ref, start, stored_ref):
    return jnp.dot(
        lhs_ref[start : start + BLOCK, :], stored_ref[...], preferred_element_type=jnp.float32
    ).astype(jnp.bfloat16)


def first_gradient(widths, pieces, stored):
    width = widths[0]
    total, hidden = stored.shape
    group = len(pieces)
    sent = width - LEFT * BLOCK

    def kernel(*refs):
        row_refs = refs[:group]
        stored_ref, grad_ref, place_ref, spare_ref, lhs_ref, held_ref, sems = refs[group:]
        places = place_of(row_refs, width, total)
        for r in range(group):
            place_ref[r] = places[r]
        pack_rows(row_refs, places, lhs_ref)
        copies = []
        for index, start in enumerate(range(0, sent, BLOCK)):
            held_ref[start : start + BLOCK, :] = product(lhs_ref, start, stored_ref)
            copy = pltpu.make_async_copy(
                held_ref.at[pl.ds(start, BLOCK)],
                grad_ref.at[pl.ds(start, BLOCK)],
                sems.at[index],
            )
            copy.start()
            copies.append(copy)
        for start in range(sent, width, BLOCK):
            spare_ref[start - sent : start - sent + BLOCK, :] = product(lhs_ref, start, stored_ref)
        for copy in copies:
            copy.wait()

    return pl.pallas_call(
        kernel,
        in_specs=[VMEM] * (group + 1),
        out_specs=[ANY, VMEM, VMEM],
        out_shape=[
            jax.ShapeDtypeStruct((sum(widths), hidden), jnp.bfloat16),
            pltpu.VMEM((group, total, CAP), jnp.bfloat16),
            pltpu.VMEM((LEFT * BLOCK, hidden), jnp.bfloat16),
        ],
        scratch_shapes=[
            pltpu.VMEM((width, total), jnp.bfloat16),
            pltpu.VMEM((sent, hidden), jnp.bfloat16),
            pltpu.SemaphoreType.DMA((sent // BLOCK,)),
        ],
        compiler_params=pltpu.CompilerParams(vmem_limit_bytes=20 * MIB),
        name="gradient0",
    )(*pieces, stored)


def second_gradient(widths, pieces, stored, gradient, place, spare):
    width = widths[1]
    base = widths[0]
    total, hidden = stored.shape
    group = len(pieces)
    left = LEFT * BLOCK

    def kernel(*refs):
        row_refs = refs[:group]
        stored_ref, place_ref, spare_ref, _, grad_ref, lhs_ref, held_ref, sems = refs[group:]
        copies = []
        for index, start in enumerate(range(0, left, BLOCK)):
            copy = pltpu.make_async_copy(
                spare_ref.at[pl.ds(start, BLOCK)],
                grad_ref.at[pl.ds(base - left + start, BLOCK)],
                sems.at[index],
            )
            copy.start()
            copies.append(copy)
        pack_rows(row_refs, [place_ref[r] for r in range(group)], lhs_ref)
        for index, start in enumerate(range(0, width, BLOCK)):
            held_ref[start : start + BLOCK, :] = product(lhs_ref, start, stored_ref)
            copy = pltpu.make_async_copy(
                held_ref.at[pl.ds(start, BLOCK)],
                grad_ref.at[pl.ds(base + start, BLOCK)],
                sems.at[LEFT + index],
            )
            copy.start()
            copies.append(copy)
        for copy in copies:
            copy.wait()

    return pl.pallas_call(
        kernel,
        in_specs=[VMEM] * (group + 3) + [ANY],
        out_specs=ANY,
        out_shape=jax.ShapeDtypeStruct((sum(widths), hidden), jnp.bfloat16),
        input_output_aliases={group + 3: 0},
        scratch_shapes=[
            pltpu.VMEM((width, total), jnp.bfloat16),
            pltpu.VMEM((width, hidden), jnp.bfloat16),
            pltpu.SemaphoreType.DMA((LEFT + width // BLOCK,)),
        ],
        compiler_params=pltpu.CompilerParams(vmem_limit_bytes=20 * MIB),
        name="gradient1",
    )(*pieces, stored, place, spare, gradient)


def partner(index, r, group):
    if group & (group - 1):
        return (index + r) % group
    return index ^ r


def per_device(out_cotangent, block_output, router_logits, keep_flags, router_weight, activated):
    cotangent = out_cotangent[0]
    stored = activated[0]
    segments = lax.axis_size("segment")
    group = lax.axis_size("tok")
    halves = lax.axis_size("mp")
    widths = widths_of(cotangent.shape[1])

    back = [(i, (i - 1) % segments) for i in range(segments)]
    came = lax.ppermute(cotangent, "segment", back)
    *rows, score_part, weight, held = prepare(
        cotangent, block_output[0], router_logits, keep_flags, router_weight, stored
    )
    pieces = []
    for index in range(PIECES):
        pieces.append(
            [rows[index]]
            + [
                lax.ppermute(rows[index], "tok", [(partner(i, r, group), i) for i in range(group)])
                for r in range(1, group)
            ]
        )
    score = score_part
    for r in range(1, halves):
        score = score + lax.ppermute(
            score_part, "mp", [(i, (i + r) % halves) for i in range(halves)]
        )
    tokens = score.shape[1]
    small = lax.ppermute(
        jnp.concatenate([score, weight], axis=1), "segment", back
    )
    gradient, place, spare = first_gradient(widths, pieces[0], held)
    gradient = second_gradient(widths, pieces[1], held, gradient, place, spare)
    received = (
        came.astype(jnp.float32) + small[0, :tokens, None] * small[:, tokens:]
    ).astype(jnp.bfloat16)
    received = jnp.where(lax.axis_index("segment") == segments - 1, 0, received)
    return (received[None], gradient[None])


def solution(mesh):
    in_specs = (
        P("segment", "tok", "mp"),
        P("segment", "tok", "mp"),
        P("segment", "tok"),
        P("segment", "tok"),
        P("segment", "mp"),
        P("segment", None, "tok"),
    )
    out_specs = (P("segment", "tok", "mp"), P("segment", "mp", "tok"))
    return jax.shard_map(
        per_device, mesh=mesh, in_specs=in_specs, out_specs=out_specs, check_vma=False
    )
```

```python
import jax
import jax.numpy as jnp
from jax import lax
from jax.experimental import pallas as pl
from jax.experimental.pallas import tpu as pltpu
from jax.sharding import PartitionSpec as P


CAP = 48
LANES = 128
BLOCK = 128
FIRST = 6
LEFT = 3
MIB = 1024 * 1024

VMEM = pl.BlockSpec(memory_space=pltpu.VMEM)
ANY = pl.BlockSpec(memory_space=pl.ANY)
HBM = pl.BlockSpec(memory_space=pltpu.HBM)


def prepare_kernel(cot_hbm, out_hbm, logit_hbm, keep_hbm, weight_hbm, stored_hbm, *refs):
    rows_ref, score_ref, weight_ref, stored_ref, cot_ref, out_ref, logit_ref, keep_ref, sems = refs
    pairs = [
        (logit_hbm, logit_ref),
        (keep_hbm, keep_ref),
        (cot_hbm, cot_ref),
        (out_hbm, out_ref),
        (weight_hbm, weight_ref),
        (stored_hbm, stored_ref),
    ]
    copies = [
        pltpu.make_async_copy(source, target, sems.at[index])
        for index, (source, target) in enumerate(pairs)
    ]
    for copy in copies:
        copy.start()
    tokens = cot_ref.shape[0]
    upper = (
        lax.broadcasted_iota(jnp.int32, (tokens, tokens), 0)
        <= lax.broadcasted_iota(jnp.int32, (tokens, tokens), 1)
    ).astype(jnp.float32).astype(jnp.bfloat16)
    copies[0].wait()
    copies[1].wait()
    keep = keep_ref[...]
    gate = jax.nn.sigmoid(logit_ref[...])
    keep_half = jnp.broadcast_to(keep.astype(jnp.float32), (16, tokens)).astype(jnp.bfloat16)
    rank = jnp.dot(keep_half, upper, preferred_element_type=jnp.float32)[:1]
    slot = lax.broadcasted_iota(jnp.int32, (CAP, tokens), 0) + 1
    chosen = (rank.astype(jnp.int32) == slot) & (keep > 0)
    gate_column = jnp.sum(jnp.where(chosen, gate, 0.0), axis=1, keepdims=True)
    chooser = jnp.where(chosen, 1.0, 0.0).astype(jnp.bfloat16)
    count = jnp.sum(keep.astype(jnp.float32), axis=1, keepdims=True)
    copies[2].wait()
    width = cot_ref.shape[1]
    picked = jnp.dot(chooser, cot_ref[...], preferred_element_type=jnp.float32)
    rows_ref[:, :width] = (picked * gate_column).astype(jnp.bfloat16)
    rows_ref[:, width:] = jnp.broadcast_to(count, (CAP, LANES)).astype(jnp.bfloat16)
    copies[3].wait()
    folded = jnp.zeros((tokens, LANES), jnp.float32)
    for start in range(0, cot_ref.shape[1], LANES):
        folded = folded + (
            cot_ref[:, start : start + LANES].astype(jnp.float32)
            * out_ref[:, start : start + LANES].astype(jnp.float32)
        )
    part = jnp.sum(folded.T, axis=0, keepdims=True)
    score_ref[...] = keep.astype(jnp.float32) * part * gate * (1.0 - gate)
    copies[4].wait()
    copies[5].wait()


def prepare(cotangent, output, logits, keep_row, weight, stored):
    operands = (cotangent, output, logits, keep_row, weight, stored)
    return pl.pallas_call(
        prepare_kernel,
        in_specs=[HBM] * 6,
        out_specs=[VMEM] * 5,
        out_shape=[
            pltpu.VMEM((CAP, cotangent.shape[1] + LANES), jnp.bfloat16),
            pltpu.VMEM(logits.shape, jnp.float32),
            pltpu.VMEM(weight.shape, jnp.float32),
            pltpu.VMEM(stored.shape, jnp.bfloat16),
            pltpu.VMEM(cotangent.shape, jnp.bfloat16),
        ],
        scratch_shapes=[
            pltpu.VMEM(output.shape, jnp.bfloat16),
            pltpu.VMEM(logits.shape, jnp.float32),
            pltpu.VMEM(keep_row.shape, jnp.int32),
            pltpu.SemaphoreType.DMA((6,)),
        ],
        compiler_params=pltpu.CompilerParams(vmem_limit_bytes=8 * MIB),
        name="prepare",
    )(*[pltpu.with_memory_space_constraint(x, pltpu.HBM) for x in operands])


def input_gradient(cotangent, scores, weight):
    tokens = cotangent.shape[0]

    def kernel(cot_ref, weight_ref, *refs):
        *score_refs, dx_ref = refs
        score = score_refs[0][...]
        for ref in score_refs[1:]:
            score = score + ref[...]
        column = jnp.broadcast_to(score, (LANES, tokens)).T
        for start in range(0, cot_ref.shape[1], LANES):
            lanes = slice(start, start + LANES)
            dx_ref[:, lanes] = (
                cot_ref[:, lanes].astype(jnp.float32) + column * weight_ref[:, lanes]
            ).astype(jnp.bfloat16)

    return pl.pallas_call(
        kernel,
        in_specs=[VMEM] * (2 + len(scores)),
        out_specs=VMEM,
        out_shape=pltpu.VMEM(cotangent.shape, jnp.bfloat16),
        compiler_params=pltpu.CompilerParams(vmem_limit_bytes=4 * MIB),
        name="input_gradient",
    )(cotangent, weight, *scores)


def light_rows(total):
    return min(CAP, total - CAP)


def mask_of(phase, half, phases):
    return 1 << ((phase + half) % phases)


def widths_of(features):
    first = features * FIRST // 16 // BLOCK * BLOCK
    return first, features - first


def merge(own, came, light, split):
    rows, width = own.shape
    heavy = CAP - light
    lights = rows - heavy
    features = width - LANES
    if split:
        first, second = widths_of(features)
        parts = [[(0, first), (features, LANES)], [(first, second)]]
    else:
        parts = [[(0, width)]]

    def kernel(own_ref, came_ref, *merged_refs):
        for ref, part in zip(merged_refs, parts):
            at = 0
            for start, size in part:
                source, target = slice(start, start + size), slice(at, at + size)
                ref[:lights, target] = own_ref[:lights, source]
                ref[lights : 2 * lights, target] = came_ref[:lights, source]
                if heavy:
                    ref[2 * lights :, target] = own_ref[lights:, source] + came_ref[lights:, source]
                at += size

    return pl.pallas_call(
        kernel,
        in_specs=[VMEM] * 2,
        out_specs=[VMEM] * len(parts),
        out_shape=[
            pltpu.VMEM((rows + lights, sum(size for _, size in part)), jnp.bfloat16)
            for part in parts
        ],
        compiler_params=pltpu.CompilerParams(vmem_limit_bytes=4 * MIB),
        name="merge",
    )(own, came)


def places_of(states, group, halves, total, width):
    light = light_rows(total)
    heavy = CAP - light
    phases = group.bit_length() - 1
    each = group // len(states)
    me, half = lax.axis_index("tok"), lax.axis_index("mp")
    counts, owners = [], []
    for chunk in range(group):
        ref = states[chunk // each]
        row = chunk % each * light
        counts.append(ref[row : row + 1, width : width + 1].astype(jnp.float32).astype(jnp.int32))
        moved = 0
        for m in range(halves):
            mask = sum(
                mask_of(p, m, phases) for p in range(phases) if chunk >> p & 1
            )
            moved = moved + jnp.where(half == m, mask, 0)
        owners.append(lax.bitwise_xor(me, moved))
    offsets = []
    for chunk in range(group):
        offset = jnp.zeros_like(counts[0])
        for other in range(group):
            if other != chunk:
                ahead = (owners[other] < owners[chunk]).astype(jnp.int32)
                offset = offset + counts[other] * ahead
        offsets.append(offset)
    first = jnp.zeros_like(counts[0])
    extra = jnp.zeros_like(counts[0])
    for count, offset in zip(counts, offsets):
        first = first + jnp.where(count > light, offset + light, 0)
        extra = extra + jnp.where(count > light, count - light, 0)
    slots = each * light + heavy
    lane = lax.broadcasted_iota(jnp.int32, (1, slots), 1)
    target = lax.broadcasted_iota(jnp.int32, (total, slots), 0)
    places = []
    for state in range(len(states)):
        start = jnp.broadcast_to(first - each * light, (1, slots))
        valid = lane - each * light < extra
        for local in range(each):
            chunk = state * each + local
            here = (lane >= local * light) & (lane < (local + 1) * light)
            start = jnp.where(here, offsets[chunk] - local * light, start)
            valid = jnp.where(here, (lane - local * light < counts[chunk]).astype(jnp.int32), valid.astype(jnp.int32)) > 0
        wanted = jnp.where(valid, start + lane, -1)
        places.append(jnp.where(wanted == target, 1.0, 0.0).astype(jnp.bfloat16))
    return places


def pack_rows(places, state_refs, lhs_ref):
    width = lhs_ref.shape[0]
    packed = None
    for place, ref in zip(places, state_refs):
        one = jnp.dot(place, ref[:, :width], preferred_element_type=jnp.float32)
        packed = one if packed is None else packed + one
    lhs_ref[...] = packed.T.astype(jnp.bfloat16)


def product(lhs_ref, start, stored_ref):
    return jnp.dot(
        lhs_ref[start : start + BLOCK, :], stored_ref[...], preferred_element_type=jnp.float32
    ).astype(jnp.bfloat16)


def send_block(source_ref, start, grad_ref, base, sem):
    copy = pltpu.make_async_copy(
        source_ref.at[pl.ds(start, BLOCK)], grad_ref.at[pl.ds(base + start, BLOCK)], sem
    )
    copy.start()
    return copy


def first_gradient(states, stored, features, group, halves):
    width = states[0].shape[1] - LANES
    total, hidden = stored.shape
    slots = states[0].shape[0]
    left = min(LEFT * BLOCK, width - BLOCK)
    sent = width - left

    def kernel(*refs):
        state_refs = refs[: len(states)]
        stored_ref, grad_ref, place_ref, spare_ref, lhs_ref, held_ref, sems = refs[len(states) :]
        places = places_of(state_refs, group, halves, total, width)
        for index, place in enumerate(places):
            place_ref[index] = place
        pack_rows(places, state_refs, lhs_ref)
        copies = []
        for index, start in enumerate(range(0, sent, BLOCK)):
            held_ref[start : start + BLOCK, :] = product(lhs_ref, start, stored_ref)
            copies.append(send_block(held_ref, start, grad_ref, 0, sems.at[index]))
        for start in range(sent, width, BLOCK):
            spare_ref[start - sent : start - sent + BLOCK, :] = product(lhs_ref, start, stored_ref)
        for copy in copies:
            copy.wait()

    return pl.pallas_call(
        kernel,
        in_specs=[VMEM] * (len(states) + 1),
        out_specs=[ANY, VMEM, VMEM],
        out_shape=[
            jax.ShapeDtypeStruct((features, hidden), jnp.bfloat16),
            pltpu.VMEM((len(states), total, slots), jnp.bfloat16),
            pltpu.VMEM((left, hidden), jnp.bfloat16),
        ],
        scratch_shapes=[
            pltpu.VMEM((width, total), jnp.bfloat16),
            pltpu.VMEM((sent, hidden), jnp.bfloat16),
            pltpu.SemaphoreType.DMA((sent // BLOCK,)),
        ],
        compiler_params=pltpu.CompilerParams(vmem_limit_bytes=24 * MIB),
        name="gradient0",
    )(*states, stored)


def second_gradient(states, stored, gradient, place, spare):
    width = states[0].shape[1]
    total, hidden = stored.shape
    features = gradient.shape[0]
    base = features - width
    left = spare.shape[0]

    def kernel(*refs):
        state_refs = refs[: len(states)]
        stored_ref, place_ref, spare_ref, _, grad_ref, lhs_ref, held_ref, sems = refs[
            len(states) :
        ]
        copies = []
        for index, start in enumerate(range(0, left, BLOCK)):
            copies.append(send_block(spare_ref, start, grad_ref, base - left, sems.at[index]))
        pack_rows([place_ref[index] for index in range(len(states))], state_refs, lhs_ref)
        for index, start in enumerate(range(0, width, BLOCK), left // BLOCK):
            held_ref[start : start + BLOCK, :] = product(lhs_ref, start, stored_ref)
            copies.append(send_block(held_ref, start, grad_ref, base, sems.at[index]))
        for copy in copies:
            copy.wait()

    return pl.pallas_call(
        kernel,
        in_specs=[VMEM] * (len(states) + 3) + [ANY],
        out_specs=ANY,
        out_shape=jax.ShapeDtypeStruct(gradient.shape, jnp.bfloat16),
        input_output_aliases={len(states) + 3: 0},
        scratch_shapes=[
            pltpu.VMEM((width, total), jnp.bfloat16),
            pltpu.VMEM((width, hidden), jnp.bfloat16),
            pltpu.SemaphoreType.DMA(((left + width) // BLOCK,)),
        ],
        compiler_params=pltpu.CompilerParams(vmem_limit_bytes=24 * MIB),
        name="gradient1",
    )(*states, stored, place, spare, gradient)


def per_device(out_cotangent, block_output, router_logits, keep_flags, router_weight, activated):
    cotangent = out_cotangent[0]
    stored = activated[0]
    segments = lax.axis_size("segment")
    group = lax.axis_size("tok")
    halves = lax.axis_size("mp")
    back = [(i, i - 1) for i in range(1, segments)]

    phases = group.bit_length() - 1
    light = light_rows(stored.shape[0])

    def exchange(rows, phase):
        pairs = [
            (t * halves + m, (t ^ mask_of(phase, m, phases)) * halves + m)
            for t in range(group)
            for m in range(halves)
        ]
        return lax.ppermute(rows, ("tok", "mp"), pairs)

    rows, score, weight, held, cot = prepare(
        cotangent, block_output[0], router_logits, keep_flags, router_weight, stored
    )
    scores = [score] + [
        lax.ppermute(score, "mp", [(i, (i + r) % halves) for i in range(halves)])
        for r in range(1, halves)
    ]
    dx = input_gradient(cot, scores, weight)
    received = lax.ppermute(dx, "segment", back)
    for phase in range(phases - 1):
        came = exchange(rows, phase)
        merged = merge(rows, came, light, phase == phases - 2)
        rows = merged[0]
    pieces = [[rows, exchange(rows, phases - 1)] for rows in merged]
    gradient, place, spare = first_gradient(pieces[0], held, cotangent.shape[1], group, halves)
    gradient = second_gradient(pieces[1], held, gradient, place, spare)
    return (received[None], gradient[None])


def solution(mesh):
    in_specs = (
        P("segment", "tok", "mp"),
        P("segment", "tok", "mp"),
        P("segment", "tok"),
        P("segment", "tok"),
        P("segment", "mp"),
        P("segment", None, "tok"),
    )
    out_specs = (P("segment", "tok", "mp"), P("segment", "mp", "tok"))
    return jax.shard_map(
        per_device, mesh=mesh, in_specs=in_specs, out_specs=out_specs, check_vma=False
    )
```

```python
import jax
import jax.numpy as jnp
from jax import lax
from jax.experimental import pallas as pl
from jax.experimental.pallas import tpu as pltpu
from jax.sharding import PartitionSpec as P


CAP = 48
LANES = 128
BLOCK = 128
FIRST = 7
LEFT = 2
MIB = 1024 * 1024

VMEM = pl.BlockSpec(memory_space=pltpu.VMEM)
ANY = pl.BlockSpec(memory_space=pl.ANY)
HBM = pl.BlockSpec(memory_space=pltpu.HBM)


def widths_of(features):
    first = features * FIRST // 16 // BLOCK * BLOCK
    return first, features - first


def prepare_kernel(cot_hbm, out_hbm, logit_hbm, keep_hbm, weight_hbm, stored_hbm, *refs):
    first_ref, second_ref, score_ref, weight_ref, stored_ref, cot_ref, *refs = refs
    out_ref, logit_ref, keep_ref, sems = refs
    pairs = [
        (logit_hbm, logit_ref),
        (keep_hbm, keep_ref),
        (cot_hbm, cot_ref),
        (out_hbm, out_ref),
        (weight_hbm, weight_ref),
        (stored_hbm, stored_ref),
    ]
    copies = [
        pltpu.make_async_copy(source, target, sems.at[index])
        for index, (source, target) in enumerate(pairs)
    ]
    for copy in copies:
        copy.start()
    tokens = cot_ref.shape[0]
    upper = (
        lax.broadcasted_iota(jnp.int32, (tokens, tokens), 0)
        <= lax.broadcasted_iota(jnp.int32, (tokens, tokens), 1)
    ).astype(jnp.float32).astype(jnp.bfloat16)
    copies[0].wait()
    copies[1].wait()
    keep = keep_ref[...]
    gate = jax.nn.sigmoid(logit_ref[...])
    keep_half = jnp.broadcast_to(keep.astype(jnp.float32), (16, tokens)).astype(jnp.bfloat16)
    rank = jnp.dot(keep_half, upper, preferred_element_type=jnp.float32)[:1]
    slot = lax.broadcasted_iota(jnp.int32, (CAP, tokens), 0) + 1
    chosen = (rank.astype(jnp.int32) == slot) & (keep > 0)
    gate_column = jnp.sum(jnp.where(chosen, gate, 0.0), axis=1, keepdims=True)
    chooser = jnp.where(chosen, 1.0, 0.0).astype(jnp.bfloat16)
    count = jnp.sum(keep.astype(jnp.float32), axis=1, keepdims=True)
    copies[2].wait()
    copies[3].wait()
    width = cot_ref.shape[1]
    folded = jnp.zeros((tokens, LANES), jnp.float32)
    for start in range(0, width, LANES):
        lanes = slice(start, start + LANES)
        folded = folded + cot_ref[:, lanes].astype(jnp.float32) * out_ref[:, lanes].astype(
            jnp.float32
        )
    picked = jnp.dot(chooser, cot_ref[...], preferred_element_type=jnp.float32)
    picked = (picked * gate_column).astype(jnp.bfloat16)
    first = first_ref.shape[1] - LANES
    first_ref[:, :first] = picked[:, :first]
    first_ref[:, first:] = jnp.broadcast_to(count, (CAP, LANES)).astype(jnp.bfloat16)
    second_ref[...] = picked[:, first:]
    part = jnp.sum(folded.T, axis=0, keepdims=True)
    score_ref[...] = keep.astype(jnp.float32) * part * gate * (1.0 - gate)
    copies[4].wait()
    copies[5].wait()


def prepare(cotangent, output, logits, keep_row, weight, stored):
    operands = (cotangent, output, logits, keep_row, weight, stored)
    first, second = widths_of(cotangent.shape[1])
    return pl.pallas_call(
        prepare_kernel,
        in_specs=[HBM] * 6,
        out_specs=[VMEM] * 6,
        out_shape=[
            pltpu.VMEM((CAP, first + LANES), jnp.bfloat16),
            pltpu.VMEM((CAP, second), jnp.bfloat16),
            pltpu.VMEM(logits.shape, jnp.float32),
            pltpu.VMEM(weight.shape, jnp.float32),
            pltpu.VMEM(stored.shape, jnp.bfloat16),
            pltpu.VMEM(cotangent.shape, jnp.bfloat16),
        ],
        scratch_shapes=[
            pltpu.VMEM(output.shape, jnp.bfloat16),
            pltpu.VMEM(logits.shape, jnp.float32),
            pltpu.VMEM(keep_row.shape, jnp.int32),
            pltpu.SemaphoreType.DMA((6,)),
        ],
        compiler_params=pltpu.CompilerParams(vmem_limit_bytes=8 * MIB),
        name="prepare",
    )(*[pltpu.with_memory_space_constraint(x, pltpu.HBM) for x in operands])


def input_gradient(cotangent, scores, weight):
    tokens = cotangent.shape[0]

    def kernel(cot_ref, weight_ref, *refs):
        *score_refs, dx_ref = refs
        score = score_refs[0][...]
        for ref in score_refs[1:]:
            score = score + ref[...]
        column = jnp.broadcast_to(score, (LANES, tokens)).T
        for start in range(0, cot_ref.shape[1], LANES):
            lanes = slice(start, start + LANES)
            dx_ref[:, lanes] = (
                cot_ref[:, lanes].astype(jnp.float32) + column * weight_ref[:, lanes]
            ).astype(jnp.bfloat16)

    return pl.pallas_call(
        kernel,
        in_specs=[VMEM] * (2 + len(scores)),
        out_specs=VMEM,
        out_shape=pltpu.VMEM(cotangent.shape, jnp.bfloat16),
        compiler_params=pltpu.CompilerParams(vmem_limit_bytes=4 * MIB),
        name="input_gradient",
    )(cotangent, weight, *scores)


def settle(came_even, came_odd):
    shape = came_even.shape

    def kernel(even_ref, odd_ref, out_ref, zero_ref, sem):
        segment = lax.axis_index("segment")
        last = segment == lax.axis_size("segment") - 1
        is_even = lax.rem(segment, 2) == 0

        def place(source):
            copy = pltpu.make_async_copy(source, out_ref, sem)
            copy.start()
            copy.wait()

        @pl.when(last)
        def _():
            zero_ref[...] = jnp.zeros(shape, zero_ref.dtype)
            place(zero_ref)

        @pl.when(jnp.logical_not(last) & is_even)
        def _():
            place(even_ref)

        @pl.when(jnp.logical_not(last | is_even))
        def _():
            place(odd_ref)

    return pl.pallas_call(
        kernel,
        in_specs=[VMEM, VMEM],
        out_specs=ANY,
        out_shape=jax.ShapeDtypeStruct(shape, came_even.dtype),
        scratch_shapes=[pltpu.VMEM(shape, came_even.dtype), pltpu.SemaphoreType.DMA(())],
        compiler_params=pltpu.CompilerParams(vmem_limit_bytes=4 * MIB),
        name="settle",
    )(came_even, came_odd)


def neighbour_pairs(first, segments, halves):
    pairs = []
    for s in range(segments):
        other = s + 1 if (s - first) % 2 == 0 else s - 1
        for m in range(halves):
            if 0 <= other < segments:
                pairs.append((s * halves + m, other * halves + m))
            else:
                pairs.append((s * halves + m, s * halves + (m + 1) % halves))
    return pairs


def light_rows(total):
    return min(CAP, total - CAP)


def mask_of(phase, half, phases):
    return 1 << ((phase + half + 1) % phases)


def merge(own, came, light):
    rows, width = own.shape
    heavy = CAP - light
    lights = rows - heavy

    def kernel(own_ref, came_ref, merged_ref):
        merged_ref[:lights] = own_ref[:lights]
        merged_ref[lights : 2 * lights] = came_ref[:lights]
        if heavy:
            merged_ref[2 * lights :] = own_ref[lights:] + came_ref[lights:]

    return pl.pallas_call(
        kernel,
        in_specs=[VMEM] * 2,
        out_specs=VMEM,
        out_shape=pltpu.VMEM((rows + lights, width), jnp.bfloat16),
        compiler_params=pltpu.CompilerParams(vmem_limit_bytes=4 * MIB),
        name="merge",
    )(own, came)


def places_of(states, group, halves, total, width):
    light = light_rows(total)
    heavy = CAP - light
    phases = group.bit_length() - 1
    each = group // len(states)
    me, half = lax.axis_index("tok"), lax.axis_index("mp")
    counts, owners = [], []
    for chunk in range(group):
        ref = states[chunk // each]
        row = chunk % each * light
        counts.append(ref[row : row + 1, width : width + 1].astype(jnp.float32).astype(jnp.int32))
        moved = 0
        for m in range(halves):
            mask = sum(
                mask_of(p, m, phases) for p in range(phases) if chunk >> p & 1
            )
            moved = moved + jnp.where(half == m, mask, 0)
        owners.append(lax.bitwise_xor(me, moved))
    offsets = []
    for chunk in range(group):
        offset = jnp.zeros_like(counts[0])
        for other in range(group):
            if other != chunk:
                ahead = (owners[other] < owners[chunk]).astype(jnp.int32)
                offset = offset + counts[other] * ahead
        offsets.append(offset)
    first = jnp.zeros_like(counts[0])
    extra = jnp.zeros_like(counts[0])
    for count, offset in zip(counts, offsets):
        first = first + jnp.where(count > light, offset + light, 0)
        extra = extra + jnp.where(count > light, count - light, 0)
    slots = each * light + heavy
    lane = lax.broadcasted_iota(jnp.int32, (1, slots), 1)
    target = lax.broadcasted_iota(jnp.int32, (total, slots), 0)
    places = []
    for state in range(len(states)):
        start = jnp.broadcast_to(first - each * light, (1, slots))
        valid = lane - each * light < extra
        for local in range(each):
            chunk = state * each + local
            here = (lane >= local * light) & (lane < (local + 1) * light)
            start = jnp.where(here, offsets[chunk] - local * light, start)
            valid = jnp.where(here, (lane - local * light < counts[chunk]).astype(jnp.int32), valid.astype(jnp.int32)) > 0
        wanted = jnp.where(valid, start + lane, -1)
        places.append(jnp.where(wanted == target, 1.0, 0.0).astype(jnp.bfloat16))
    return places


def pack_rows(places, state_refs, lhs_ref):
    width = lhs_ref.shape[0]
    packed = None
    for place, ref in zip(places, state_refs):
        one = jnp.dot(place, ref[:, :width], preferred_element_type=jnp.float32)
        packed = one if packed is None else packed + one
    lhs_ref[...] = packed.T.astype(jnp.bfloat16)


def product(lhs_ref, start, stored_ref):
    return jnp.dot(
        lhs_ref[start : start + BLOCK, :], stored_ref[...], preferred_element_type=jnp.float32
    ).astype(jnp.bfloat16)


def send_block(source_ref, start, grad_ref, base, sem):
    copy = pltpu.make_async_copy(
        source_ref.at[pl.ds(start, BLOCK)], grad_ref.at[pl.ds(base + start, BLOCK)], sem
    )
    copy.start()
    return copy


def first_gradient(states, stored, features, group, halves):
    width = states[0].shape[1] - LANES
    total, hidden = stored.shape
    slots = states[0].shape[0]
    left = min(LEFT * BLOCK, width - BLOCK)
    sent = width - left

    def kernel(*refs):
        state_refs = refs[: len(states)]
        stored_ref, grad_ref, place_ref, spare_ref, lhs_ref, held_ref, sems = refs[len(states) :]
        places = places_of(state_refs, group, halves, total, width)
        for index, place in enumerate(places):
            place_ref[index] = place
        pack_rows(places, state_refs, lhs_ref)
        copies = []
        for index, start in enumerate(range(0, sent, BLOCK)):
            held_ref[start : start + BLOCK, :] = product(lhs_ref, start, stored_ref)
            copies.append(send_block(held_ref, start, grad_ref, 0, sems.at[index]))
        for start in range(sent, width, BLOCK):
            spare_ref[start - sent : start - sent + BLOCK, :] = product(lhs_ref, start, stored_ref)
        for copy in copies:
            copy.wait()

    return pl.pallas_call(
        kernel,
        in_specs=[VMEM] * (len(states) + 1),
        out_specs=[ANY, VMEM, VMEM],
        out_shape=[
            jax.ShapeDtypeStruct((features, hidden), jnp.bfloat16),
            pltpu.VMEM((len(states), total, slots), jnp.bfloat16),
            pltpu.VMEM((left, hidden), jnp.bfloat16),
        ],
        scratch_shapes=[
            pltpu.VMEM((width, total), jnp.bfloat16),
            pltpu.VMEM((sent, hidden), jnp.bfloat16),
            pltpu.SemaphoreType.DMA((sent // BLOCK,)),
        ],
        compiler_params=pltpu.CompilerParams(vmem_limit_bytes=24 * MIB),
        name="gradient0",
    )(*states, stored)


def second_gradient(states, stored, gradient, place, spare):
    width = states[0].shape[1]
    total, hidden = stored.shape
    features = gradient.shape[0]
    base = features - width
    left = spare.shape[0]

    def kernel(*refs):
        state_refs = refs[: len(states)]
        stored_ref, place_ref, spare_ref, _, grad_ref, lhs_ref, held_ref, sems = refs[
            len(states) :
        ]
        copies = []
        for index, start in enumerate(range(0, left, BLOCK)):
            copies.append(send_block(spare_ref, start, grad_ref, base - left, sems.at[index]))
        pack_rows([place_ref[index] for index in range(len(states))], state_refs, lhs_ref)
        for index, start in enumerate(range(0, width, BLOCK), left // BLOCK):
            held_ref[start : start + BLOCK, :] = product(lhs_ref, start, stored_ref)
            copies.append(send_block(held_ref, start, grad_ref, base, sems.at[index]))
        for copy in copies:
            copy.wait()

    return pl.pallas_call(
        kernel,
        in_specs=[VMEM] * (len(states) + 3) + [ANY],
        out_specs=ANY,
        out_shape=jax.ShapeDtypeStruct(gradient.shape, jnp.bfloat16),
        input_output_aliases={len(states) + 3: 0},
        scratch_shapes=[
            pltpu.VMEM((width, total), jnp.bfloat16),
            pltpu.VMEM((width, hidden), jnp.bfloat16),
            pltpu.SemaphoreType.DMA(((left + width) // BLOCK,)),
        ],
        compiler_params=pltpu.CompilerParams(vmem_limit_bytes=24 * MIB),
        name="gradient1",
    )(*states, stored, place, spare, gradient)


def per_device(out_cotangent, block_output, router_logits, keep_flags, router_weight, activated):
    cotangent = out_cotangent[0]
    stored = activated[0]
    segments = lax.axis_size("segment")
    group = lax.axis_size("tok")
    halves = lax.axis_size("mp")

    phases = group.bit_length() - 1
    light = light_rows(stored.shape[0])

    def exchange(rows, phase):
        pairs = [
            (t * halves + m, (t ^ mask_of(phase, m, phases)) * halves + m)
            for t in range(group)
            for m in range(halves)
        ]
        return lax.ppermute(rows, ("tok", "mp"), pairs)

    *rows, score, weight, held, cot = prepare(
        cotangent, block_output[0], router_logits, keep_flags, router_weight, stored
    )
    scores = [score] + [
        lax.ppermute(score, "mp", [(i, (i + r) % halves) for i in range(halves)])
        for r in range(1, halves)
    ]
    dx = input_gradient(cot, scores, weight)
    relayed = []
    for first in range(2):
        relayed.append(
            lax.ppermute(
                dx, ("segment", "mp"), neighbour_pairs(first, segments, halves)
            )
        )
    for phase in range(phases - 1):
        arrived = [exchange(rows[piece], phase) for piece in range(2)]
        rows = [merge(rows[piece], arrived[piece], light) for piece in range(2)]
    pieces = [[rows[piece], exchange(rows[piece], phases - 1)] for piece in range(2)]
    gradient, place, spare = first_gradient(pieces[0], held, cotangent.shape[1], group, halves)
    gradient = second_gradient(pieces[1], held, gradient, place, spare)
    received = settle(*relayed)
    return (received[None], gradient[None])


def solution(mesh):
    in_specs = (
        P("segment", "tok", "mp"),
        P("segment", "tok", "mp"),
        P("segment", "tok"),
        P("segment", "tok"),
        P("segment", "mp"),
        P("segment", None, "tok"),
    )
    out_specs = (P("segment", "tok", "mp"), P("segment", "mp", "tok"))
    return jax.shard_map(
        per_device, mesh=mesh, in_specs=in_specs, out_specs=out_specs, check_vma=False
    )
```
